256 devices in a mesh: tm: 8 (over z), par: 32 (over x, y, core).
Axes of the slice: x: 4, y: 4, z: 8, core: 2. Of those that a mesh axis runs over, the one named last changes fastest.
Arguments:
- kernel: bfloat16 [128, 256, 4096], P('tm', None, 'par'), may hold values from -0.015625 to 0.015625
- history: bfloat16 [128, 4096, 128], P('tm', 'par'), may hold values from -6 to 6
- arrivals: bfloat16 [2, 16, 4096, 128], P(None, 'tm', 'par'), may hold values from -6 to 6
Outputs:
- observations: bfloat16 [2, 16, 256, 128], P(None, None, ('tm', 'par'))
The draws below stay inside these ranges and needn't reach their ends.
All inputs are finite; a program needn't handle non-finite values.
Results may differ from the reference program's by a relative error of at most 0.014.
Values may be sent and summed in bfloat16 or wider, within the bound.
No kernel may reach another device: no remote copies, remote signals or barrier semaphores. Data moves between devices by JAX's collectives and lax.ppermute only.
A program may use at most 64 MiB of HBM per device.

```python
import jax
import jax.numpy as jnp
from jax import lax

TB = 16
NF = 17
SENS = 256
FIELDS = 128
STEPS = 2
NT = 128
NP = 4096
N_TM = 8


def strengthened(entries, stream_key, source, target, shards_of, factor):
    owner, partner = [(jnp.arange(entries.shape[axis_at]) // (entries.shape[axis_at] // shards_of)).reshape([-1 if axis == axis_at else 1 for axis in range(entries.ndim)]) for axis_at in (source, target)]
    chosen = jax.random.permutation(stream_key, shards_of)[partner]
    strong = (owner == chosen) | (owner == (partner + shards_of // 2) % shards_of)
    return jnp.where(strong, factor * entries, entries)


def levels(own_key, dims, cuts, least, top_value):
    def one(position, parts):
        draws = jax.random.uniform(jax.random.fold_in(jax.random.fold_in(own_key, 6), position), (parts,), jnp.float32, least / len(cuts), top_value / len(cuts))
        return jnp.repeat(jnp.exp(draws), dims[position] // parts).reshape((-1,) + (1,) * (len(dims) - position - 1))

    gain = one(*cuts[0])
    for cut in cuts[1:]:
        gain = gain * one(*cut)
    return gain


def normal_values(rng, shape, scale, limit, cuts=(), kind=jnp.bfloat16):
    loudness = levels(rng, shape, cuts, -0.22, 0.18) if cuts else 1.0
    result = jax.random.normal(rng, shape, jnp.float32) * scale * loudness
    return jnp.minimum(jnp.maximum(result, -limit), limit).astype(kind)


def noise_with(key, shape, spread, reach, shards, heavy, kind=jnp.bfloat16):
    drawn = spread * jax.random.normal(key, shape, jnp.float32)
    if shards:
        drawn = drawn * levels(key, shape, shards, -0.22, 0.18)
    return jnp.clip(strengthened(drawn, jax.random.fold_in(key, 3), *heavy), -reach, reach).astype(kind)


def setup_inputs(seed: int = 0) -> dict:
    streams_of = jax.random.split(jax.random.key(seed), 4)
    return {
        "kernel": noise_with(streams_of[0], (NT, SENS, NP), (NT * NP) ** -0.5, 0.015625, ((0, 8), (2, 32)), (2, 1, 32, 2.75)),
        "history": normal_values(streams_of[1], (NT, NP, FIELDS), 1.0, 6.0, ((0, 8), (1, 32))),
        "arrivals": normal_values(streams_of[2], (STEPS, TB, NP, FIELDS), 1.0, 6.0, ((1, 8), (2, 32))),
    }


def rounded(values):
    narrow = values.astype(jnp.bfloat16)
    narrow = lax.optimization_barrier(narrow)
    return narrow.astype(jnp.float32)


def reference(kernel, history, arrivals):
    length = 2 * TB
    ordered = jnp.concatenate([history.reshape(N_TM, TB, NP, FIELDS)[::-1], arrivals], 0)
    accum_shape = (STEPS, NF, SENS, FIELDS)

    def one_lag(totals, lag_index):
        real_acc, imag_acc = totals
        first_row = (lag_index * TB).astype(jnp.int32)
        lag_block = lax.dynamic_slice_in_dim(kernel, first_row, TB, 0).astype(jnp.float32)
        spectrum = jnp.fft.rfft(lag_block, n=length, axis=0)
        kernel_real_component = rounded(jnp.real(spectrum))
        kernel_imaginary = rounded(jnp.imag(spectrum))
        for step_index in range(STEPS):
            first_block = (N_TM - 1 + step_index - lag_index).astype(jnp.int32)
            window = lax.dynamic_slice_in_dim(ordered, first_block, 2, 0)
            window = window.reshape(length, NP, FIELDS).astype(jnp.float32)
            window_spec = jnp.fft.rfft(window, axis=0)
            window_real_component = rounded(jnp.real(window_spec))
            window_imaginary = rounded(jnp.imag(window_spec))
            real_component = jnp.einsum("njy,nyv->njv", kernel_real_component, window_real_component, precision=lax.Precision.HIGHEST)
            real_component = real_component - jnp.einsum("njy,nyv->njv", kernel_imaginary, window_imaginary, precision=lax.Precision.HIGHEST)
            imaginary_component = jnp.einsum("njy,nyv->njv", kernel_real_component, window_imaginary, precision=lax.Precision.HIGHEST)
            imaginary_component = imaginary_component + jnp.einsum("njy,nyv->njv", kernel_imaginary, window_real_component, precision=lax.Precision.HIGHEST)
            real_acc = real_acc.at[step_index].add(real_component)
            imag_acc = imag_acc.at[step_index].add(imaginary_component)
        return (real_acc, imag_acc), None

    zeros_start = jnp.zeros(accum_shape, jnp.float32)
    (real_acc, imag_acc), unused = lax.scan(one_lag, (zeros_start, zeros_start), jnp.arange(N_TM, dtype=jnp.int32))
    signal = jnp.fft.irfft(lax.complex(real_acc, imag_acc), n=length, axis=1)
    return signal[:, TB:].astype(jnp.bfloat16)
```

```python
import jax
import jax.numpy as jnp
from jax import lax
from jax.experimental import pallas as pl
from jax.experimental.pallas import tpu as pltpu
from jax.sharding import Mesh
from jax.sharding import PartitionSpec as P

PAR = ("x", "y", "c")
EVERY = ("z", "x", "y", "c")


def ordered_kernel(position, kernel, ordered):
    lags, sensors, params = kernel.shape
    planes = position[1]
    half = sensors // 2
    row = lax.broadcasted_iota(jnp.int32, (sensors, sensors), 0)
    col = lax.broadcasted_iota(jnp.int32, (sensors, sensors), 1)
    other = (row >= half).astype(jnp.int32)
    place = row - half * other
    core = position[0] + other - 2 * position[0] * other
    planes = 8
    sensor = (place % planes) * (sensors // planes) + (place // planes) * 2 + core
    select = (col == sensor).astype(jnp.bfloat16)
    for lag in range(lags):
        rows = jnp.dot(select, kernel[lag], preferred_element_type=jnp.float32)
        ordered[:, lag * params : (lag + 1) * params] = rows.astype(jnp.bfloat16)


def convolve(position, ordered, older, shifted, shifted_twice, arrived, mine, theirs, times):
    block, params, fields = older.shape
    steps = arrived.shape[1]
    rows_each = arrived.shape[2]
    sensors = ordered.shape[0]
    total = (steps + 1) * block
    plane = position[0]

    def put(time, value):
        times[(total - 1 - time) * params : (total - time) * params, :fields] = value
        if time:
            times[(total - time) * params : (total - time + 1) * params, fields:] = value

    for time in range(total):
        which, at = divmod(time, block)
        if which == 0:
            put(time, older[at])
            continue
        near = arrived[at // rows_each, which - 1, at % rows_each]
        if which == 1:
            put(time, jnp.where(plane == 0, near, shifted[at]))
        else:
            near_one = arrived[at // rows_each, 0, at % rows_each]
            late = jnp.where(plane == 1, near_one, shifted_twice[at])
            put(time, jnp.where(plane == 0, near, late))

    half = sensors // 2

    def pair(index, carry):
        first = index * 2
        start = pl.multiple_of((total - 1 - block - first) * params, params)
        window = times[pl.ds(start, block * params), :]
        sums = jnp.dot(ordered[...], window, preferred_element_type=jnp.float32)
        sums = sums.astype(jnp.bfloat16)
        for odd in range(2):
            part = sums[:, odd * fields : (odd + 1) * fields]
            mine[:, first + odd] = part[:half].reshape(mine.shape[0], mine.shape[2], fields)
            theirs[:, first + odd] = part[half:].reshape(mine.shape[0], mine.shape[2], fields)
        return carry

    lax.fori_loop(0, steps * block // 2, pair, 0)


def shift(array, axis, by):
    size = lax.axis_size(axis)
    return lax.ppermute(array, axis, [(i, (i + by) % size) for i in range(size)])


def exchange(parts, axis):
    return lax.all_to_all(parts, axis, split_axis=0, concat_axis=0, tiled=True)


def per_device(kernel, history, arrivals):
    block, sensors, params = kernel.shape
    steps, rows_each, _, fields = arrivals.shape
    planes = lax.axis_size("z")
    chips = lax.axis_size("x") * lax.axis_size("y")
    plane = lax.axis_index("z")
    core = lax.axis_index("c")
    vmem = pl.BlockSpec(memory_space=pltpu.VMEM)
    smem = pl.BlockSpec(memory_space=pltpu.SMEM)

    arrived = exchange(jnp.broadcast_to(arrivals, (planes, *arrivals.shape)), "z")
    shifted = shift(history, "z", 1)
    shifted_twice = shift(shifted, "z", 1)
    ordered = pl.pallas_call(
        ordered_kernel,
        out_shape=jax.ShapeDtypeStruct((sensors, block * params), jnp.bfloat16),
        in_specs=[smem, vmem],
        out_specs=vmem,
        name="ordered_kernel",
    )(jnp.stack([core, plane]).astype(jnp.int32), kernel)
    part = jax.ShapeDtypeStruct((chips, steps * block, planes, fields), jnp.bfloat16)
    mine, theirs = pl.pallas_call(
        convolve,
        out_shape=(part, part),
        in_specs=[smem] + [vmem] * 5,
        out_specs=(vmem, vmem),
        scratch_shapes=[pltpu.VMEM(((steps + 1) * block * params, 2 * fields), jnp.bfloat16)],
        compiler_params=pltpu.CompilerParams(vmem_limit_bytes=24 * 1024 * 1024),
        name="convolve",
    )(plane.astype(jnp.int32).reshape(1), ordered, history, shifted, shifted_twice, arrived)
    paired = mine.astype(jnp.float32) + shift(theirs, "c", 1).astype(jnp.float32)
    in_plane = exchange(paired.astype(jnp.bfloat16), ("x", "y"))
    in_plane = in_plane.astype(jnp.float32).sum(axis=0)
    across = exchange(jnp.moveaxis(in_plane, 1, 0).astype(jnp.bfloat16), "z")
    across = across.astype(jnp.float32).sum(axis=0).astype(jnp.bfloat16)
    return across.reshape(steps, block, 1, fields)


def solution(mesh):
    split = Mesh(mesh.devices.reshape(mesh.shape["tm"], 4, 4, 2), EVERY)
    placed = (P("z", None, PAR), P("z", PAR, None), P(None, "z", PAR, None))
    return jax.shard_map(
        per_device,
        mesh=split,
        in_specs=placed,
        out_specs=P(None, None, EVERY, None),
        check_vma=False,
    )
```

```python
import jax
import jax.numpy as jnp
from jax import lax
from jax.experimental import pallas as pl
from jax.experimental.pallas import tpu as pltpu
from jax.sharding import Mesh
from jax.sharding import PartitionSpec as P

PAR = ("x", "y", "c")
EVERY = ("z", "x", "y", "c")
VMEM = pl.BlockSpec(memory_space=pltpu.VMEM)
SMEM = pl.BlockSpec(memory_space=pltpu.SMEM)
LIMIT = pltpu.CompilerParams(vmem_limit_bytes=24 * 1024 * 1024)


def work(flops, nbytes):
    return pl.CostEstimate(flops=flops, bytes_accessed=nbytes, transcendentals=0)


def upper_part(ordered, older, upper, times):
    block, params, fields = older.shape
    last = block - 2
    for time in range(1, block):
        if time <= last:
            times[(last - time) * params : (last - time + 1) * params, :fields] = older[time]
        if time >= 2:
            at = last + 1 - time
            times[at * params : (at + 1) * params, fields:] = older[time]
    for pair in range(block // 2 - 1):
        lag = (2 * pair + 2) * params
        upper[pair] = jnp.dot(
            ordered[:, lag:], times[: block * params - lag], preferred_element_type=jnp.float32
        )


def first_part(core, kernel, older, ordered, upper, times):
    lags, sensors, params = kernel.shape
    planes = 8
    half = sensors // 2
    row = lax.broadcasted_iota(jnp.int32, (sensors, sensors), 0)
    col = lax.broadcasted_iota(jnp.int32, (sensors, sensors), 1)
    other = (row >= half).astype(jnp.int32)
    place = row - half * other
    parity = core[0] + other - 2 * core[0] * other
    sensor = (place % planes) * (sensors // planes) + (place // planes) * 2 + parity
    select = (col == sensor).astype(jnp.bfloat16)
    for lag in range(lags):
        rows = jnp.dot(select, kernel[lag], preferred_element_type=jnp.float32)
        ordered[:, lag * params : (lag + 1) * params] = rows.astype(jnp.bfloat16)
    upper_part(ordered, older, upper, times)


def lower_part(ordered, older, newer, upper, mine, theirs, times):
    block, params, fields = newer.shape
    half = ordered.shape[0] // 2
    for time in range(-1, block):
        value = newer[time] if time >= 0 else older[block - 1]
        at = block - 2 - time
        if time <= block - 2:
            times[at * params : (at + 1) * params, :fields] = value
        if time >= 0:
            times[(at + 1) * params : (at + 2) * params, fields:] = value
    for pair in range(block // 2):
        lag = (2 * pair + 2) * params
        sums = jnp.dot(
            ordered[:, :lag], times[block * params - lag :], preferred_element_type=jnp.float32
        )
        if pair < block // 2 - 1:
            sums = sums + upper[pair]
        sums = sums.astype(jnp.bfloat16)
        for odd in range(2):
            part = sums[:, odd * fields : (odd + 1) * fields]
            mine[:, 2 * pair + odd] = part[:half].reshape(mine.shape[0], mine.shape[2], fields)
            theirs[:, 2 * pair + odd] = part[half:].reshape(mine.shape[0], mine.shape[2], fields)


def ring(array, axis, by):
    size = lax.axis_size(axis)
    return lax.ppermute(array, axis, [(i, (i + by) % size) for i in range(size)])


def onward(array, axis):
    return lax.ppermute(array, axis, [(i, i + 1) for i in range(lax.axis_size(axis) - 1)])


def exchange(parts, axis):
    return lax.all_to_all(parts, axis, split_axis=0, concat_axis=0, tiled=True)


def observed(kernel, history, arrivals):
    block, sensors, params = kernel.shape
    steps, _, _, fields = arrivals.shape
    planes = lax.axis_size("z")
    chips = lax.axis_size("x") * lax.axis_size("y")
    plane = lax.axis_index("z")
    core = lax.axis_index("c").astype(jnp.int32).reshape(1)
    pairs = (block // 2 - 1, sensors, 2 * fields)
    scratch = [pltpu.VMEM((block * params, 2 * fields), jnp.bfloat16)]
    part = jax.ShapeDtypeStruct((chips, block, planes, fields), jnp.bfloat16)

    shifted = onward(history, "z")
    sources = [4, 3, 5, 2, 6, 1, 7]
    pieces = {0: arrivals}
    for source in sources:
        pieces[source] = lax.ppermute(arrivals, "z", [(source, 0)])

    def newer_of(step, received):
        newest = jnp.concatenate([pieces[i][step] for i in range(planes)], 0)
        return jnp.where(plane == 0, newest, received)

    ordered, upper = pl.pallas_call(
        first_part,
        out_shape=(
            jax.ShapeDtypeStruct((sensors, block * params), jnp.bfloat16),
            jax.ShapeDtypeStruct(pairs, jnp.float32),
        ),
        in_specs=[SMEM, VMEM, VMEM],
        out_specs=(VMEM, VMEM),
        scratch_shapes=scratch,
        compiler_params=LIMIT,
        cost_estimate=work(2 * 10**9, 4 * 10**6),
        name="first_part",
    )(core, kernel, history)

    def lower(older, newer, upper):
        return pl.pallas_call(
            lower_part,
            out_shape=(part, part),
            in_specs=[VMEM] * 4,
            out_specs=(VMEM, VMEM),
            scratch_shapes=scratch,
            compiler_params=LIMIT,
            cost_estimate=work(2 * 10**9, 6 * 10**6),
            name="lower_part",
        )(ordered, older, newer, upper)

    def in_plane(mine, theirs):
        received = ring(theirs, "c", 1)
        paired = (mine.astype(jnp.float32) + received.astype(jnp.float32)).astype(jnp.bfloat16)
        return exchange(paired, ("x", "y"))

    newer = newer_of(0, shifted)
    shifted_twice = onward(newer, "z")
    mine, theirs = lower(history, newer, upper)
    arrived_first = in_plane(mine, theirs)
    upper = pl.pallas_call(
        upper_part,
        out_shape=jax.ShapeDtypeStruct(pairs, jnp.float32),
        in_specs=[VMEM] * 2,
        out_specs=VMEM,
        scratch_shapes=scratch,
        compiler_params=LIMIT,
        cost_estimate=work(10**9, 4 * 10**6),
        name="upper_part",
    )(ordered, newer)
    newest = newer_of(1, shifted_twice)
    mine, theirs = lower(newer, newest, upper)
    arrived_second = in_plane(mine, theirs)
    summed = jnp.concatenate(
        [part.astype(jnp.float32).sum(axis=0) for part in (arrived_first, arrived_second)], 0
    )
    across = exchange(jnp.moveaxis(summed, 1, 0).astype(jnp.bfloat16), "z")
    across = across.astype(jnp.float32).sum(axis=0).astype(jnp.bfloat16)
    return across.reshape(steps, block, 1, fields)


def solution(mesh):
    split = Mesh(mesh.devices.reshape(mesh.shape["tm"], 4, 4, 2), EVERY)
    placed = (P("z", None, PAR), P("z", PAR, None), P(None, "z", PAR, None))
    return jax.shard_map(
        observed,
        mesh=split,
        in_specs=placed,
        out_specs=P(None, None, EVERY, None),
        check_vma=False,
    )
```

```python
import jax
import jax.numpy as jnp
from jax import lax
from jax.experimental import pallas as pl
from jax.experimental.pallas import tpu as pltpu
from jax.sharding import Mesh
from jax.sharding import PartitionSpec as P

PAR = ("x", "y", "c")
EVERY = ("z", "x", "y", "c")
VMEM = pl.BlockSpec(memory_space=pltpu.VMEM)
HBM = pl.BlockSpec(memory_space=pltpu.HBM)
LIMIT = pltpu.CompilerParams(vmem_limit_bytes=8 * 1024 * 1024)


def work(flops, nbytes):
    return pl.CostEstimate(flops=flops, bytes_accessed=nbytes, transcendentals=0)


def upper_part(ordered, older, upper, times):
    block, params, fields = older.shape
    last = block - 2
    for time in range(1, block):
        if time <= last:
            times[(last - time) * params : (last - time + 1) * params, :fields] = older[time]
        if time >= 2:
            at = last + 1 - time
            times[at * params : (at + 1) * params, fields:] = older[time]
    for pair in range(block // 2 - 1):
        lag = (2 * pair + 2) * params
        upper[pair] = jnp.dot(
            ordered[:, lag:], times[: block * params - lag], preferred_element_type=jnp.float32
        )


def first_part(kernel_hbm, older_hbm, ordered, upper, times, kernel, older, arrived):
    copies = [
        pltpu.make_async_copy(kernel_hbm.at[lag], kernel.at[lag], arrived.at[lag])
        for lag in range(kernel.shape[0])
    ]
    copies.append(pltpu.make_async_copy(older_hbm, older, arrived.at[kernel.shape[0]]))
    for copy in copies:
        copy.start()
    lags, sensors, params = kernel.shape
    planes = 8
    half = sensors // 2
    row = lax.broadcasted_iota(jnp.int32, (sensors, sensors), 0)
    col = lax.broadcasted_iota(jnp.int32, (sensors, sensors), 1)
    other = (row >= half).astype(jnp.int32)
    place = row - half * other
    core = lax.axis_index("c")
    parity = core + other - 2 * core * other
    sensor = (place % planes) * (sensors // planes) + (place // planes) * 2 + parity
    select = (col == sensor).astype(jnp.bfloat16)
    for lag in range(lags):
        copies[lag].wait()
        rows = jnp.dot(select, kernel[lag], preferred_element_type=jnp.float32)
        ordered[:, lag * params : (lag + 1) * params] = rows.astype(jnp.bfloat16)
    copies[lags].wait()
    upper_part(ordered, older, upper, times)


def lower_part(ordered, older, received, upper, *refs):
    *late, mine, theirs, times = refs
    block, params, fields = received.shape
    here = lax.axis_index("z") == 0
    half = ordered.shape[0] // 2
    for time in range(-1, block):
        value = received[time] if time >= 0 else older[block - 1]
        if late and time >= 0:
            value = jnp.where(here, late[0][time], value)
        at = block - 2 - time
        if time <= block - 2:
            times[at * params : (at + 1) * params, :fields] = value
        if time >= 0:
            times[(at + 1) * params : (at + 2) * params, fields:] = value
    for pair in range(block // 2):
        lag = (2 * pair + 2) * params
        sums = jnp.dot(
            ordered[:, :lag], times[block * params - lag :], preferred_element_type=jnp.float32
        )
        if pair < block // 2 - 1:
            sums = sums + upper[pair]
        sums = sums.astype(jnp.bfloat16)
        for odd in range(2):
            part = sums[:, odd * fields : (odd + 1) * fields]
            mine[:, 2 * pair + odd] = part[:half].reshape(mine.shape[0], mine.shape[2], fields)
            theirs[:, 2 * pair + odd] = part[half:].reshape(mine.shape[0], mine.shape[2], fields)


def newer_part(*refs):
    *pieces, received, newer, late = refs
    here = lax.axis_index("z") == 0
    each = pieces[0].shape[1]
    for time in range(newer.shape[0]):
        piece = pieces[time // each]
        newer[time] = jnp.where(here, piece[0, time % each], received[time])
        late[time] = piece[1, time % each]


def pair_part(mine, received, paired):
    for chip in range(mine.shape[0]):
        both = mine[chip].astype(jnp.float32) + received[chip].astype(jnp.float32)
        paired[chip] = both.astype(jnp.bfloat16)


def plane_part(arrived, summed):
    for time in range(arrived.shape[1]):
        total = arrived[0, time].astype(jnp.float32)
        for chip in range(1, arrived.shape[0]):
            total = total + arrived[chip, time].astype(jnp.float32)
        summed[time] = total.astype(jnp.bfloat16)


def ring(array, axis, by):
    size = lax.axis_size(axis)
    return lax.ppermute(array, axis, [(i, (i + by) % size) for i in range(size)])


def onward(array, axis):
    return lax.ppermute(array, axis, [(i, i + 1) for i in range(lax.axis_size(axis) - 1)])


def exchange(parts, axis):
    return lax.all_to_all(parts, axis, split_axis=0, concat_axis=0, tiled=True)


def observed(kernel, history, arrivals):
    block, sensors, params = kernel.shape
    steps, _, _, fields = arrivals.shape
    planes = lax.axis_size("z")
    chips = lax.axis_size("x") * lax.axis_size("y")
    pairs = (block // 2 - 1, sensors, 2 * fields)
    scratch = [pltpu.VMEM((block * params, 2 * fields), jnp.bfloat16)]
    part = jax.ShapeDtypeStruct((chips, block, planes, fields), jnp.bfloat16)

    shifted = onward(history, "z")
    sources = [4, 3, 5, 2, 6, 1, 7]
    pieces = {0: arrivals}
    for source in sources:
        pieces[source] = lax.ppermute(arrivals, "z", [(source, 0)])

    ordered, upper = pl.pallas_call(
        first_part,
        out_shape=(
            jax.ShapeDtypeStruct((sensors, block * params), jnp.bfloat16),
            jax.ShapeDtypeStruct(pairs, jnp.float32),
        ),
        in_specs=[HBM, HBM],
        out_specs=(VMEM, VMEM),
        scratch_shapes=scratch
        + [
            pltpu.VMEM(kernel.shape, jnp.bfloat16),
            pltpu.VMEM(history.shape, jnp.bfloat16),
            pltpu.SemaphoreType.DMA((block + 1,)),
        ],
        compiler_params=LIMIT,
        cost_estimate=work(2 * 10**9, 4 * 10**6),
        name="first_part",
    )(kernel, history)

    def lower(older, received, upper, *late):
        return pl.pallas_call(
            lower_part,
            out_shape=(part, part),
            in_specs=[VMEM] * (4 + len(late)),
            out_specs=(VMEM, VMEM),
            scratch_shapes=scratch,
            compiler_params=LIMIT,
            cost_estimate=work(2 * 10**9, 6 * 10**6),
        )(ordered, older, received, upper, *late)

    def in_plane(mine, theirs):
        received = ring(theirs, "c", 1)
        paired = pl.pallas_call(
            pair_part,
            out_shape=part,
            in_specs=[VMEM] * 2,
            out_specs=VMEM,
            compiler_params=LIMIT,
            name="pair_part",
        )(mine, received)
        arrived = exchange(paired, ("x", "y"))
        return pl.pallas_call(
            plane_part,
            out_shape=jax.ShapeDtypeStruct((block, planes, fields), jnp.bfloat16),
            in_specs=[VMEM],
            out_specs=VMEM,
            compiler_params=LIMIT,
            name="plane_part",
        )(arrived)

    newer, late = pl.pallas_call(
        newer_part,
        out_shape=(jax.ShapeDtypeStruct(shifted.shape, jnp.bfloat16),) * 2,
        in_specs=[VMEM] * (planes + 1),
        out_specs=(VMEM, VMEM),
        compiler_params=LIMIT,
        name="newer_part",
    )(*[pieces[i] for i in range(planes)], shifted)
    shifted_twice = onward(newer, "z")
    mine, theirs = lower(history, newer, upper)
    arrived_first = in_plane(mine, theirs)
    upper = pl.pallas_call(
        upper_part,
        out_shape=jax.ShapeDtypeStruct(pairs, jnp.float32),
        in_specs=[VMEM] * 2,
        out_specs=VMEM,
        scratch_shapes=scratch,
        compiler_params=LIMIT,
        cost_estimate=work(10**9, 4 * 10**6),
        name="upper_part",
    )(ordered, newer)
    mine, theirs = lower(newer, shifted_twice, upper, late)
    arrived_second = in_plane(mine, theirs)
    summed = jnp.concatenate([arrived_first, arrived_second], 0)
    across = exchange(jnp.moveaxis(summed, 1, 0), "z")
    across = across.astype(jnp.float32).sum(axis=0).astype(jnp.bfloat16)
    return across.reshape(steps, block, 1, fields)


def solution(mesh):
    split = Mesh(mesh.devices.reshape(mesh.shape["tm"], 4, 4, 2), EVERY)
    placed = (P("z", None, PAR), P("z", PAR, None), P(None, "z", PAR, None))
    return jax.shard_map(
        observed,
        mesh=split,
        in_specs=placed,
        out_specs=P(None, None, EVERY, None),
        check_vma=False,
    )
```

```python
import functools

import jax
import jax.numpy as jnp
from jax import lax
from jax.experimental import pallas as pl
from jax.experimental.pallas import tpu as pltpu
from jax.sharding import Mesh
from jax.sharding import PartitionSpec as P

ORDER = (5, 6, 7, 4, 3, 2, 1)
PAR = ("x", "y", "c")
EVERY = ("z", "x", "y", "c")
VMEM = pl.BlockSpec(memory_space=pltpu.VMEM)
LIMIT = pltpu.CompilerParams(vmem_limit_bytes=8 * 1024 * 1024)


def work(flops, nbytes):
    return pl.CostEstimate(flops=flops, bytes_accessed=nbytes, transcendentals=0)


def upper_part(ordered, older, upper, times):
    block, params, fields = older.shape
    last = block - 2
    for time in range(1, block):
        if time <= last:
            times[(last - time) * params : (last - time + 1) * params, :fields] = older[time]
        if time >= 2:
            at = last + 1 - time
            times[at * params : (at + 1) * params, fields:] = older[time]
    for pair in range(block // 2 - 1):
        lag = (2 * pair + 2) * params
        upper[pair] = jnp.dot(
            ordered[:, lag:], times[: block * params - lag], preferred_element_type=jnp.float32
        )


def order_rows(kernel, ordered):
    lags, sensors, params = kernel.shape
    planes = 8
    half = sensors // 2
    row = lax.broadcasted_iota(jnp.int32, (sensors, sensors), 0)
    col = lax.broadcasted_iota(jnp.int32, (sensors, sensors), 1)
    other = (row >= half).astype(jnp.int32)
    place = row - half * other
    core = lax.axis_index("c")
    parity = core + other - 2 * core * other
    sensor = (place % planes) * (sensors // planes) + (place // planes) * 2 + parity
    select = (col == sensor).astype(jnp.bfloat16)
    for lag in range(lags):
        rows = jnp.dot(select, kernel[lag], preferred_element_type=jnp.float32)
        ordered[:, lag * params : (lag + 1) * params] = rows.astype(jnp.bfloat16)


def first_part(kernel, older, ordered, leading, upper, times):
    order_rows(kernel, ordered)
    leading[...] = ordered[:, : leading.shape[1]]
    upper_part(ordered, older, upper, times)


def windows(value, low, high, params, fields, times):
    for time in range(low, high + 2):
        if time <= high:
            times[(high - time) * params : (high - time + 1) * params, :fields] = value(time)
        if time > low:
            at = high + 1 - time
            times[at * params : (at + 1) * params, fields:] = value(time)


def put(sums, pair, mine, theirs):
    half = sums.shape[0] // 2
    fields = sums.shape[1] // 2
    sums = sums.astype(jnp.bfloat16)
    for odd in range(2):
        part = sums[:, odd * fields : (odd + 1) * fields]
        mine[:, 2 * pair + odd] = part[:half].reshape(mine.shape[0], mine.shape[2], fields)
        theirs[:, 2 * pair + odd] = part[half:].reshape(mine.shape[0], mine.shape[2], fields)


def second_part(
    ordered, following, older, newer, head, last, mine, theirs, ahead, behind, arrivals
):
    block, params, fields = older.shape
    lags = following.shape[1] // params
    plane = lax.axis_index("z")

    def after(first, then):
        return lambda time: first[time] if time < block else then[time - block]

    windows(after(older, newer), lags + 1, 2 * block - 2, params, fields, ahead)

    def conv(left, right, pair):
        start = (block - 2 - 2 * pair) * params
        return jnp.dot(
            left, right[start : start + left.shape[1]], preferred_element_type=jnp.float32
        )

    @pl.when(plane != 0)
    def _():
        windows(after(newer, head), 1, 2 * block - 2 - lags, params, fields, behind)
        for pair in range(block // 2):
            sums = conv(following[...], ahead, pair)
            sums = sums + conv(ordered[:, lags * params :], behind, pair)
            put(sums, pair, mine, theirs)

    @pl.when(plane == 0)
    def _():
        windows(after(newer, last), 1, 2 * block - 2, params, fields, arrivals)
        for pair in range(block // 2):
            sums = conv(following[...], ahead, pair) + conv(ordered[...], arrivals, pair)
            put(sums, pair, mine, theirs)


def lower_part(ordered, older, newer, upper, mine, theirs, times):
    block, params, fields = newer.shape
    for time in range(-1, block):
        value = newer[time] if time >= 0 else older[block - 1]
        at = block - 2 - time
        if time <= block - 2:
            times[at * params : (at + 1) * params, :fields] = value
        if time >= 0:
            times[(at + 1) * params : (at + 2) * params, fields:] = value
    for pair in range(block // 2):
        lag = (2 * pair + 2) * params
        sums = jnp.dot(
            ordered[:, :lag], times[block * params - lag :], preferred_element_type=jnp.float32
        )
        if pair < block // 2 - 1:
            sums = sums + upper[pair]
        put(sums, pair, mine, theirs)


def head_part(*refs):
    *pieces, received, head = refs
    here = lax.axis_index("z") == 0
    each = pieces[0].shape[1]
    for time in range(head.shape[0]):
        piece = pieces[time // each]
        head[time] = jnp.where(here, piece[0, time % each], received[time])


def newer_part(*refs):
    *pieces, received, newer, last = refs
    here = lax.axis_index("z") == 0
    each = pieces[0].shape[1]
    for time in range(newer.shape[0]):
        piece = pieces[time // each]
        newer[time] = jnp.where(here, piece[0, time % each], received[time])
        last[time] = piece[1, time % each]


def pair_part(step, mine, received, *refs):
    paired = refs[-1]
    block = mine.shape[1]
    for chip in range(mine.shape[0]):
        both = mine[chip].astype(jnp.float32) + received[chip].astype(jnp.float32)
        paired[chip, step * block : (step + 1) * block] = both.astype(jnp.bfloat16)


def plane_part(arrived, summed):
    for time in range(arrived.shape[1]):
        total = arrived[0, time].astype(jnp.float32)
        for chip in range(1, arrived.shape[0]):
            total = total + arrived[chip, time].astype(jnp.float32)
        summed[time] = total.astype(jnp.bfloat16)


def ring(array, axis, by):
    size = lax.axis_size(axis)
    return lax.ppermute(array, axis, [(i, (i + by) % size) for i in range(size)])


def onward(array, axis, by):
    size = lax.axis_size(axis)
    return lax.ppermute(array, axis, [(i, i + by) for i in range(size) if 0 <= i + by < size])


def exchange(parts, axis):
    return lax.all_to_all(parts, axis, split_axis=0, concat_axis=0, tiled=True)


def observed(kernel, history, arrivals):
    block, sensors, params = kernel.shape
    steps, _, _, fields = arrivals.shape
    planes = lax.axis_size("z")
    chips = lax.axis_size("x") * lax.axis_size("y")
    pairs = (block // 2 - 1, sensors, 2 * fields)
    scratch = [pltpu.VMEM((block * params, 2 * fields), jnp.bfloat16)]
    part = jax.ShapeDtypeStruct((chips, block, planes, fields), jnp.bfloat16)

    shifted = onward(history, "z", 1)
    pieces = [arrivals] + [None] * (planes - 1)
    for source in ORDER:
        pieces[source] = lax.ppermute(arrivals, "z", [(source, 0)])

    ordered, leading, upper = pl.pallas_call(
        first_part,
        out_shape=(
            jax.ShapeDtypeStruct((sensors, block * params), jnp.bfloat16),
            jax.ShapeDtypeStruct((sensors, block // 2 * params), jnp.bfloat16),
            jax.ShapeDtypeStruct(pairs, jnp.float32),
        ),
        in_specs=[VMEM, VMEM],
        out_specs=(VMEM, VMEM, VMEM),
        scratch_shapes=scratch,
        compiler_params=LIMIT,
        cost_estimate=work(2 * 10**9, 4 * 10**6),
        name="first_part",
    )(kernel, history)

    following = onward(leading, "z", -1)

    def pair(step, mine, theirs, *paired):
        received = ring(theirs, "c", 1)
        return pl.pallas_call(
            functools.partial(pair_part, step),
            out_shape=jax.ShapeDtypeStruct((chips, steps * block, planes, fields), jnp.bfloat16),
            in_specs=[VMEM] * (2 + len(paired)),
            out_specs=VMEM,
            input_output_aliases={2: 0} if paired else {},
            compiler_params=LIMIT,
            name="pair_part",
        )(mine, received, *paired)

    near = planes // 2
    head = pl.pallas_call(
        head_part,
        out_shape=jax.ShapeDtypeStruct((block // 2, params, fields), jnp.bfloat16),
        in_specs=[VMEM] * (near + 1),
        out_specs=VMEM,
        compiler_params=LIMIT,
        name="head_part",
    )(*pieces[:near], shifted)
    head_twice = onward(head, "z", 1)
    newer, last = pl.pallas_call(
        newer_part,
        out_shape=(jax.ShapeDtypeStruct(shifted.shape, jnp.bfloat16),) * 2,
        in_specs=[VMEM] * (planes + 1),
        out_specs=(VMEM, VMEM),
        compiler_params=LIMIT,
        name="newer_part",
    )(*pieces, shifted)
    mine, theirs = pl.pallas_call(
        lower_part,
        out_shape=(part, part),
        in_specs=[VMEM] * 4,
        out_specs=(VMEM, VMEM),
        scratch_shapes=scratch,
        compiler_params=LIMIT,
        cost_estimate=work(2 * 10**9, 6 * 10**6),
        name="lower_part",
    )(ordered, history, newer, upper)
    paired = pair(0, mine, theirs)
    width = 2 * fields
    mine, theirs = pl.pallas_call(
        second_part,
        out_shape=(part, part),
        in_specs=[VMEM] * 6,
        out_specs=(VMEM, VMEM),
        scratch_shapes=[
            pltpu.VMEM(((3 * block // 2 - 2) * params, width), jnp.bfloat16),
            pltpu.VMEM(((3 * block // 2 - 2) * params, width), jnp.bfloat16),
            pltpu.VMEM(((2 * block - 2) * params, width), jnp.bfloat16),
        ],
        compiler_params=pltpu.CompilerParams(vmem_limit_bytes=12 * 1024 * 1024),
        cost_estimate=work(4 * 10**9, 8 * 10**6),
        name="second_part",
    )(ordered, following, history, newer, head_twice, last)
    paired = pair(1, mine, theirs, paired)
    arrived = exchange(paired, ("x", "y"))
    summed = pl.pallas_call(
        plane_part,
        out_shape=jax.ShapeDtypeStruct((steps * block, planes, fields), jnp.bfloat16),
        in_specs=[VMEM],
        out_specs=VMEM,
        compiler_params=LIMIT,
        name="plane_part",
    )(arrived)
    across = exchange(jnp.moveaxis(summed, 1, 0), "z")
    across = across.astype(jnp.float32).sum(axis=0).astype(jnp.bfloat16)
    return across.reshape(steps, block, 1, fields)


def solution(mesh):
    split = Mesh(mesh.devices.reshape(mesh.shape["tm"], 4, 4, 2), EVERY)
    placed = (P("z", None, PAR), P("z", PAR, None), P(None, "z", PAR, None))
    return jax.shard_map(
        observed,
        mesh=split,
        in_specs=placed,
        out_specs=P(None, None, EVERY, None),
        check_vma=False,
    )
```

```python
import functools

import jax
import jax.numpy as jnp
from jax import lax
from jax.experimental import pallas as pl
from jax.experimental.pallas import tpu as pltpu
from jax.sharding import Mesh
from jax.sharding import PartitionSpec as P

SOURCES = (1, 2, 3, 5, 6, 7)
PAR = ("x", "y", "c")
EVERY = ("z", "x", "y", "c")
VMEM = pl.BlockSpec(memory_space=pltpu.VMEM)
LIMIT = pltpu.CompilerParams(vmem_limit_bytes=8 * 1024 * 1024)


def work(flops, nbytes):
    return pl.CostEstimate(flops=flops, bytes_accessed=nbytes, transcendentals=0)


def order_rows(kernel, ordered):
    lags, sensors, params = kernel.shape
    planes = 8
    half = sensors // 2
    row = lax.broadcasted_iota(jnp.int32, (sensors, sensors), 0)
    col = lax.broadcasted_iota(jnp.int32, (sensors, sensors), 1)
    other = (row >= half).astype(jnp.int32)
    place = row - half * other
    core = lax.axis_index("c")
    parity = core + other - 2 * core * other
    sensor = (place % planes) * (sensors // planes) + (place // planes) * 2 + parity
    select = (col == sensor).astype(jnp.bfloat16)
    for lag in range(lags):
        rows = jnp.dot(select, kernel[lag], preferred_element_type=jnp.float32)
        ordered[:, lag * params : (lag + 1) * params] = rows.astype(jnp.bfloat16)


def first_part(kernel, ordered, leading):
    order_rows(kernel, ordered)
    leading[...] = ordered[:, : leading.shape[1]]


def windows(value, low, high, params, fields, times):
    for time in range(low, high + 2):
        if time <= high:
            times[(high - time) * params : (high - time + 1) * params, :fields] = value(time)
        if time > low:
            at = high + 1 - time
            times[at * params : (at + 1) * params, fields:] = value(time)


def after(first, then):
    block = first.shape[0]
    return lambda time: first[time] if time < block else then[time - block]


def product(left, right, start):
    window = right[start : start + left.shape[1]]
    return jnp.dot(left, window, preferred_element_type=jnp.float32)


def put_half(sums, pair, half):
    fields = sums.shape[1] // 2
    sums = sums.astype(jnp.bfloat16)
    for odd in range(2):
        part = sums[:, odd * fields : (odd + 1) * fields]
        half[:, 2 * pair + odd] = part.reshape(half.shape[0], half.shape[2], fields)


def put(sums, pair, mine, theirs):
    count = sums.shape[0] // 2
    put_half(sums[:count], pair, mine)
    put_half(sums[count:], pair, theirs)


def second_part(
    side, ordered, following, older, newer, head, last, half, ahead, behind, arrivals
):
    block, params, fields = older.shape
    lags = following.shape[1] // params
    plane = lax.axis_index("z")
    count = ordered.shape[0] // 2
    rows = slice(side * count, (side + 1) * count)
    windows(after(older, newer), block + 1 - lags, 2 * block - 2, params, fields, ahead)

    def conv(left, right, pair):
        return product(left, right, (block - 2 - 2 * pair) * params)

    @pl.when(plane != 0)
    def _():
        windows(after(newer, head), 1, 2 * block - 2 - lags, params, fields, behind)
        for pair in range(block // 2):
            sums = conv(following[rows], ahead, pair)
            sums = sums + conv(ordered[rows, lags * params :], behind, pair)
            put_half(sums, pair, half)

    @pl.when(plane == 0)
    def _():
        windows(after(newer, last), 1, 2 * block - 2, params, fields, arrivals)
        for pair in range(block // 2):
            sums = conv(following[rows], ahead, pair) + conv(ordered[rows], arrivals, pair)
            put_half(sums, pair, half)


def step_zero(ordered, older, newer, mine, theirs, times):
    block, params, fields = newer.shape
    windows(after(older, newer), 1, 2 * block - 2, params, fields, times)
    for pair in range(block // 2):
        start = (block - 2 - 2 * pair) * params
        put(product(ordered[...], times, start), pair, mine, theirs)


def row_of(pieces, step, time):
    own, first, second, third, fifth, sixth, seventh = pieces
    source, row = divmod(time, own.shape[1])
    if source == 4:
        return third[own.shape[0] + step, row]
    return (own, first, second, third, None, fifth, sixth, seventh)[source][step, row]


def joined(own, other, both):
    both[: own.shape[0]] = own[...]
    both[own.shape[0] :] = other[...]


def head_part(*refs):
    *near, received, head = refs
    here = lax.axis_index("z") == 0
    for time in range(head.shape[0]):
        row = row_of((*near, None, None, None), 0, time)
        head[time] = jnp.where(here, row, received[time])


def newer_part(*refs):
    *pieces, received, newer, last = refs
    here = lax.axis_index("z") == 0
    for time in range(newer.shape[0]):
        newer[time] = jnp.where(here, row_of(pieces, 0, time), received[time])
        last[time] = row_of(pieces, 1, time)


def pair_part(step, mine, received, *refs):
    paired = refs[-1]
    block = mine.shape[1]
    for chip in range(mine.shape[0]):
        both = mine[chip].astype(jnp.float32) + received[chip].astype(jnp.float32)
        paired[chip, step * block : (step + 1) * block] = both.astype(jnp.bfloat16)


def plane_part(arrived, summed):
    for time in range(arrived.shape[1]):
        total = arrived[0, time].astype(jnp.float32)
        for chip in range(1, arrived.shape[0]):
            total = total + arrived[chip, time].astype(jnp.float32)
        summed[time] = total.astype(jnp.bfloat16)


def ring(array, axis, by):
    size = lax.axis_size(axis)
    return lax.ppermute(array, axis, [(i, (i + by) % size) for i in range(size)])


def onward(array, axis, by):
    size = lax.axis_size(axis)
    return lax.ppermute(array, axis, [(i, i + by) for i in range(size) if 0 <= i + by < size])


def exchange(parts, axis):
    return lax.all_to_all(parts, axis, split_axis=0, concat_axis=0, tiled=True)


def observed(kernel, history, arrivals):
    block, sensors, params = kernel.shape
    steps, _, _, fields = arrivals.shape
    planes = lax.axis_size("z")
    chips = lax.axis_size("x") * lax.axis_size("y")
    part = jax.ShapeDtypeStruct((chips, block, planes, fields), jnp.bfloat16)

    shifted = onward(history, "z", 1)
    relayed = lax.ppermute(arrivals, "z", [(4, 3)])
    both = pl.pallas_call(
        joined,
        out_shape=jax.ShapeDtypeStruct((2 * steps, *arrivals.shape[1:]), jnp.bfloat16),
        in_specs=[VMEM] * 2,
        out_specs=VMEM,
        compiler_params=LIMIT,
        name="joined",
    )(arrivals, relayed)
    pieces = [arrivals]
    for source in SOURCES:
        operand = both if source == 3 else arrivals
        pieces.append(lax.ppermute(operand, "z", [(source, 0)]))

    ordered, leading = pl.pallas_call(
        first_part,
        out_shape=(
            jax.ShapeDtypeStruct((sensors, block * params), jnp.bfloat16),
            jax.ShapeDtypeStruct((sensors, block // 2 * params), jnp.bfloat16),
        ),
        in_specs=[VMEM],
        out_specs=(VMEM, VMEM),
        compiler_params=LIMIT,
        cost_estimate=work(2 * 10**9, 4 * 10**6),
        name="first_part",
    )(kernel)

    following = onward(leading, "z", -1)

    def pair(step, mine, theirs, *paired):
        received = ring(theirs, "c", 1)
        return pl.pallas_call(
            functools.partial(pair_part, step),
            out_shape=jax.ShapeDtypeStruct((chips, steps * block, planes, fields), jnp.bfloat16),
            in_specs=[VMEM] * (2 + len(paired)),
            out_specs=VMEM,
            input_output_aliases={2: 0} if paired else {},
            compiler_params=LIMIT,
            name="pair_part",
        )(mine, received, *paired)

    near = planes // 2
    head = pl.pallas_call(
        head_part,
        out_shape=jax.ShapeDtypeStruct((block // 2, params, fields), jnp.bfloat16),
        in_specs=[VMEM] * (near + 1),
        out_specs=VMEM,
        compiler_params=LIMIT,
        name="head_part",
    )(*pieces[:near], shifted)
    head_twice = onward(head, "z", 1)
    newer, last = pl.pallas_call(
        newer_part,
        out_shape=(jax.ShapeDtypeStruct(shifted.shape, jnp.bfloat16),) * 2,
        in_specs=[VMEM] * planes,
        out_specs=(VMEM, VMEM),
        compiler_params=LIMIT,
        name="newer_part",
    )(*pieces, shifted)
    mine, theirs = pl.pallas_call(
        step_zero,
        out_shape=(part, part),
        in_specs=[VMEM] * 3,
        out_specs=(VMEM, VMEM),
        scratch_shapes=[pltpu.VMEM(((2 * block - 2) * params, 2 * fields), jnp.bfloat16)],
        compiler_params=LIMIT,
        cost_estimate=work(2 * 10**9, 6 * 10**6),
        name="step_zero",
    )(ordered, history, newer)
    paired = pair(0, mine, theirs)
    width = 2 * fields

    def second(side):
        return pl.pallas_call(
            functools.partial(second_part, side),
            out_shape=part,
            in_specs=[VMEM] * 6,
            out_specs=VMEM,
            scratch_shapes=[
                pltpu.VMEM(((3 * block // 2 - 2) * params, width), jnp.bfloat16),
                pltpu.VMEM(((3 * block // 2 - 2) * params, width), jnp.bfloat16),
                pltpu.VMEM(((2 * block - 2) * params, width), jnp.bfloat16),
            ],
            compiler_params=pltpu.CompilerParams(vmem_limit_bytes=12 * 1024 * 1024),
            cost_estimate=work(2 * 10**9, 8 * 10**6),
            name="second_part",
        )(ordered, following, history, newer, head_twice, last)

    theirs = second(1)
    mine = second(0)
    paired = pair(1, mine, theirs, paired)
    arrived = exchange(paired, ("x", "y"))
    summed = pl.pallas_call(
        plane_part,
        out_shape=jax.ShapeDtypeStruct((steps * block, planes, fields), jnp.bfloat16),
        in_specs=[VMEM],
        out_specs=VMEM,
        compiler_params=LIMIT,
        name="plane_part",
    )(arrived)
    across = exchange(jnp.moveaxis(summed, 1, 0), "z")
    across = across.astype(jnp.float32).sum(axis=0).astype(jnp.bfloat16)
    return across.reshape(steps, block, 1, fields)


def solution(mesh):
    split = Mesh(mesh.devices.reshape(mesh.shape["tm"], 4, 4, 2), EVERY)
    placed = (P("z", None, PAR), P("z", PAR, None), P(None, "z", PAR, None))
    return jax.shard_map(
        observed,
        mesh=split,
        in_specs=placed,
        out_specs=P(None, None, EVERY, None),
        check_vma=False,
    )
```

```python
import functools

import jax
import jax.numpy as jnp
from jax import lax
from jax.experimental import pallas as pl
from jax.experimental.pallas import tpu as pltpu
from jax.sharding import Mesh
from jax.sharding import PartitionSpec as P

ORDER = (5, 6, 7, 4, 3, 2, 1)
LEADING = 9
PAR = ("x", "y", "c")
EVERY = ("z", "x", "y", "c")
VMEM = pl.BlockSpec(memory_space=pltpu.VMEM)
LIMIT = pltpu.CompilerParams(vmem_limit_bytes=8 * 1024 * 1024)


def work(flops, nbytes):
    return pl.CostEstimate(flops=flops, bytes_accessed=nbytes, transcendentals=0)


def upper_part(ordered, older, upper, times):
    block, params, fields = older.shape
    last = block - 2
    for time in range(1, block):
        if time <= last:
            times[(last - time) * params : (last - time + 1) * params, :fields] = older[time]
        if time >= 2:
            at = last + 1 - time
            times[at * params : (at + 1) * params, fields:] = older[time]
    for pair in range(block // 2 - 1):
        lag = (2 * pair + 2) * params
        upper[pair] = jnp.dot(
            ordered[:, lag:], times[: block * params - lag], preferred_element_type=jnp.float32
        )


def order_rows(kernel, ordered):
    lags, sensors, params = kernel.shape
    planes = 8
    half = sensors // 2
    row = lax.broadcasted_iota(jnp.int32, (sensors, sensors), 0)
    col = lax.broadcasted_iota(jnp.int32, (sensors, sensors), 1)
    other = (row >= half).astype(jnp.int32)
    place = row - half * other
    core = lax.axis_index("c")
    parity = core + other - 2 * core * other
    sensor = (place % planes) * (sensors // planes) + (place // planes) * 2 + parity
    select = (col == sensor).astype(jnp.bfloat16)
    for lag in range(lags):
        rows = jnp.dot(select, kernel[lag], preferred_element_type=jnp.float32)
        ordered[:, lag * params : (lag + 1) * params] = rows.astype(jnp.bfloat16)


def first_part(kernel, older, ordered, leading, upper, times):
    order_rows(kernel, ordered)
    leading[...] = ordered[:, : leading.shape[1]]
    upper_part(ordered, older, upper, times)


def windows(value, low, high, params, fields, times):
    for time in range(low, high + 2):
        if time <= high:
            times[(high - time) * params : (high - time + 1) * params, :fields] = value(time)
        if time > low:
            at = high + 1 - time
            times[at * params : (at + 1) * params, fields:] = value(time)


def after(first, then):
    block = first.shape[0]
    return lambda time: first[time] if time < block else then[time - block]


def product(left, right, start):
    window = right[start : start + left.shape[1]]
    return jnp.dot(left, window, preferred_element_type=jnp.float32)


def put_half(sums, pair, half):
    fields = sums.shape[1] // 2
    sums = sums.astype(jnp.bfloat16)
    for odd in range(2):
        part = sums[:, odd * fields : (odd + 1) * fields]
        half[:, 2 * pair + odd] = part.reshape(half.shape[0], half.shape[2], fields)


def put(sums, pair, mine, theirs):
    count = sums.shape[0] // 2
    put_half(sums[:count], pair, mine)
    put_half(sums[count:], pair, theirs)


def second_part(
    side, ordered, following, older, newer, head, last, half, ahead, behind, arrivals
):
    block, params, fields = older.shape
    lags = following.shape[1] // params
    plane = lax.axis_index("z")
    count = ordered.shape[0] // 2
    rows = slice(side * count, (side + 1) * count)
    windows(after(older, newer), block + 1 - lags, 2 * block - 2, params, fields, ahead)

    def conv(left, right, pair):
        return product(left, right, (block - 2 - 2 * pair) * params)

    @pl.when(plane != 0)
    def _():
        windows(after(newer, head), 1, 2 * block - 2 - lags, params, fields, behind)
        for pair in range(block // 2):
            sums = conv(following[rows], ahead, pair)
            sums = sums + conv(ordered[rows, lags * params :], behind, pair)
            put_half(sums, pair, half)

    @pl.when(plane == 0)
    def _():
        windows(after(newer, last), 1, 2 * block - 2, params, fields, arrivals)
        for pair in range(block // 2):
            sums = conv(following[rows], ahead, pair) + conv(ordered[rows], arrivals, pair)
            put_half(sums, pair, half)


def lower_part(ordered, older, newer, upper, mine, theirs, times):
    block, params, fields = newer.shape
    for time in range(-1, block):
        value = newer[time] if time >= 0 else older[block - 1]
        at = block - 2 - time
        if time <= block - 2:
            times[at * params : (at + 1) * params, :fields] = value
        if time >= 0:
            times[(at + 1) * params : (at + 2) * params, fields:] = value
    for pair in range(block // 2):
        lag = (2 * pair + 2) * params
        sums = jnp.dot(
            ordered[:, :lag], times[block * params - lag :], preferred_element_type=jnp.float32
        )
        if pair < block // 2 - 1:
            sums = sums + upper[pair]
        put(sums, pair, mine, theirs)


def head_part(*refs):
    *pieces, received, head = refs
    here = lax.axis_index("z") == 0
    each = pieces[0].shape[1]
    for time in range(head.shape[0]):
        piece = pieces[time // each]
        head[time] = jnp.where(here, piece[0, time % each], received[time])


def newer_part(*refs):
    *pieces, received, newer, last = refs
    here = lax.axis_index("z") == 0
    each = pieces[0].shape[1]
    for time in range(newer.shape[0]):
        piece = pieces[time // each]
        newer[time] = jnp.where(here, piece[0, time % each], received[time])
        last[time] = piece[1, time % each]


def pair_part(step, mine, received, *refs):
    paired = refs[-1]
    block = mine.shape[1]
    for chip in range(mine.shape[0]):
        both = mine[chip].astype(jnp.float32) + received[chip].astype(jnp.float32)
        paired[chip, step * block : (step + 1) * block] = both.astype(jnp.bfloat16)


def plane_part(arrived, summed):
    for time in range(arrived.shape[1]):
        total = arrived[0, time].astype(jnp.float32)
        for chip in range(1, arrived.shape[0]):
            total = total + arrived[chip, time].astype(jnp.float32)
        summed[time] = total.astype(jnp.bfloat16)


def ring(array, axis, by):
    size = lax.axis_size(axis)
    return lax.ppermute(array, axis, [(i, (i + by) % size) for i in range(size)])


def onward(array, axis, by):
    size = lax.axis_size(axis)
    return lax.ppermute(array, axis, [(i, i + by) for i in range(size) if 0 <= i + by < size])


def exchange(parts, axis):
    return lax.all_to_all(parts, axis, split_axis=0, concat_axis=0, tiled=True)


def observed(kernel, history, arrivals):
    block, sensors, params = kernel.shape
    steps, _, _, fields = arrivals.shape
    planes = lax.axis_size("z")
    chips = lax.axis_size("x") * lax.axis_size("y")
    pairs = (block // 2 - 1, sensors, 2 * fields)
    scratch = [pltpu.VMEM((block * params, 2 * fields), jnp.bfloat16)]
    part = jax.ShapeDtypeStruct((chips, block, planes, fields), jnp.bfloat16)

    shifted = onward(history, "z", 1)
    pieces = [arrivals] + [None] * (planes - 1)
    for source in ORDER:
        pieces[source] = lax.ppermute(arrivals, "z", [(source, 0)])

    ordered, leading, upper = pl.pallas_call(
        first_part,
        out_shape=(
            jax.ShapeDtypeStruct((sensors, block * params), jnp.bfloat16),
            jax.ShapeDtypeStruct((sensors, LEADING * params), jnp.bfloat16),
            jax.ShapeDtypeStruct(pairs, jnp.float32),
        ),
        in_specs=[VMEM, VMEM],
        out_specs=(VMEM, VMEM, VMEM),
        scratch_shapes=scratch,
        compiler_params=LIMIT,
        cost_estimate=work(2 * 10**9, 4 * 10**6),
        name="first_part",
    )(kernel, history)

    following = onward(leading, "z", -1)

    def pair(step, mine, theirs, *paired):
        received = ring(theirs, "c", 1)
        return pl.pallas_call(
            functools.partial(pair_part, step),
            out_shape=jax.ShapeDtypeStruct((chips, steps * block, planes, fields), jnp.bfloat16),
            in_specs=[VMEM] * (2 + len(paired)),
            out_specs=VMEM,
            input_output_aliases={2: 0} if paired else {},
            compiler_params=LIMIT,
            name="pair_part",
        )(mine, received, *paired)

    near = -(-(block - LEADING) // arrivals.shape[1])
    head = pl.pallas_call(
        head_part,
        out_shape=jax.ShapeDtypeStruct((block - LEADING, params, fields), jnp.bfloat16),
        in_specs=[VMEM] * (near + 1),
        out_specs=VMEM,
        compiler_params=LIMIT,
        name="head_part",
    )(*pieces[:near], shifted)
    head_twice = onward(head, "z", 1)
    newer, last = pl.pallas_call(
        newer_part,
        out_shape=(jax.ShapeDtypeStruct(shifted.shape, jnp.bfloat16),) * 2,
        in_specs=[VMEM] * (planes + 1),
        out_specs=(VMEM, VMEM),
        compiler_params=LIMIT,
        name="newer_part",
    )(*pieces, shifted)
    mine, theirs = pl.pallas_call(
        lower_part,
        out_shape=(part, part),
        in_specs=[VMEM] * 4,
        out_specs=(VMEM, VMEM),
        scratch_shapes=scratch,
        compiler_params=LIMIT,
        cost_estimate=work(2 * 10**9, 6 * 10**6),
        name="lower_part",
    )(ordered, history, newer, upper)
    paired = pair(0, mine, theirs)
    width = 2 * fields

    def second(side):
        return pl.pallas_call(
            functools.partial(second_part, side),
            out_shape=part,
            in_specs=[VMEM] * 6,
            out_specs=VMEM,
            scratch_shapes=[
                pltpu.VMEM(((block - 2 + LEADING) * params, width), jnp.bfloat16),
                pltpu.VMEM(((2 * block - 2 - LEADING) * params, width), jnp.bfloat16),
                pltpu.VMEM(((2 * block - 2) * params, width), jnp.bfloat16),
            ],
            compiler_params=pltpu.CompilerParams(vmem_limit_bytes=12 * 1024 * 1024),
            cost_estimate=work(2 * 10**9, 8 * 10**6),
            name="second_part",
        )(ordered, following, history, newer, head_twice, last)

    theirs = second(1)
    mine = second(0)
    paired = pair(1, mine, theirs, paired)
    arrived = exchange(paired, ("x", "y"))
    summed = pl.pallas_call(
        plane_part,
        out_shape=jax.ShapeDtypeStruct((steps * block, planes, fields), jnp.bfloat16),
        in_specs=[VMEM],
        out_specs=VMEM,
        compiler_params=LIMIT,
        name="plane_part",
    )(arrived)
    across = exchange(jnp.moveaxis(summed, 1, 0), "z")
    across = across.astype(jnp.float32).sum(axis=0).astype(jnp.bfloat16)
    return across.reshape(steps, block, 1, fields)


def solution(mesh):
    split = Mesh(mesh.devices.reshape(mesh.shape["tm"], 4, 4, 2), EVERY)
    placed = (P("z", None, PAR), P("z", PAR, None), P(None, "z", PAR, None))
    return jax.shard_map(
        observed,
        mesh=split,
        in_specs=placed,
        out_specs=P(None, None, EVERY, None),
        check_vma=False,
    )
```

```python
import functools

import jax
import jax.numpy as jnp
from jax import lax
from jax.experimental import pallas as pl
from jax.experimental.pallas import tpu as pltpu
from jax.sharding import Mesh
from jax.sharding import PartitionSpec as P

ORDER = (5, 6, 7, 4, 3, 2, 1)
LEADING = 9
PAR = ("x", "y", "c")
EVERY = ("z", "x", "y", "c")
VMEM = pl.BlockSpec(memory_space=pltpu.VMEM)
LIMIT = pltpu.CompilerParams(vmem_limit_bytes=8 * 1024 * 1024)


def work(flops, nbytes):
    return pl.CostEstimate(flops=flops, bytes_accessed=nbytes, transcendentals=0)


def upper_part(ordered, older, upper, times):
    block, params, fields = older.shape
    last = block - 2
    for time in range(1, block):
        if time <= last:
            times[(last - time) * params : (last - time + 1) * params, :fields] = older[time]
        if time >= 2:
            at = last + 1 - time
            times[at * params : (at + 1) * params, fields:] = older[time]
    for pair in range(block // 2 - 1):
        lag = (2 * pair + 2) * params
        upper[pair] = jnp.dot(
            ordered[:, lag:], times[: block * params - lag], preferred_element_type=jnp.float32
        )


def order_rows(kernel, ordered):
    lags, sensors, params = kernel.shape
    planes = 8
    half = sensors // 2
    row = lax.broadcasted_iota(jnp.int32, (sensors, sensors), 0)
    col = lax.broadcasted_iota(jnp.int32, (sensors, sensors), 1)
    other = (row >= half).astype(jnp.int32)
    place = row - half * other
    core = lax.axis_index("c")
    parity = core + other - 2 * core * other
    sensor = (place % planes) * (sensors // planes) + (place // planes) * 2 + parity
    select = (col == sensor).astype(jnp.bfloat16)
    for lag in range(lags):
        rows = jnp.dot(select, kernel[lag], preferred_element_type=jnp.float32)
        ordered[:, lag * params : (lag + 1) * params] = rows.astype(jnp.bfloat16)


def first_part(kernel, older, ordered, leading, upper, times):
    order_rows(kernel, ordered)
    leading[...] = ordered[:, : leading.shape[1]]
    upper_part(ordered, older, upper, times)


def windows(value, low, high, params, fields, times):
    for time in range(low, high + 2):
        if time <= high:
            times[(high - time) * params : (high - time + 1) * params, :fields] = value(time)
        if time > low:
            at = high + 1 - time
            times[at * params : (at + 1) * params, fields:] = value(time)


def after(first, then):
    block = first.shape[0]
    return lambda time: first[time] if time < block else then[time - block]


def product(left, right, start):
    window = right[start : start + left.shape[1]]
    return jnp.dot(left, window, preferred_element_type=jnp.float32)


def put_half(sums, pair, half):
    fields = sums.shape[1] // 2
    sums = sums.astype(jnp.bfloat16)
    for odd in range(2):
        part = sums[:, odd * fields : (odd + 1) * fields]
        half[:, 2 * pair + odd] = part.reshape(half.shape[0], half.shape[2], fields)


def put(sums, pair, mine, theirs):
    count = sums.shape[0] // 2
    put_half(sums[:count], pair, mine)
    put_half(sums[count:], pair, theirs)


def second_part(side, ordered, following, ahead, *refs):
    *blocks, half, behind = refs if side else (*refs[1:], refs[0])
    block = half.shape[1]
    params = ordered.shape[1] // block
    fields = ahead.shape[1] // 2
    lags = following.shape[1] // params
    plane = lax.axis_index("z")
    count = ordered.shape[0] // 2
    rows = slice(side * count, (side + 1) * count)

    def conv(left, right, pair):
        return product(left, right, (block - 2 - 2 * pair) * params)

    @pl.when(plane != 0)
    def _():
        if blocks:
            newer, head, _ = blocks
            windows(after(newer, head), 1, 2 * block - 2 - lags, params, fields, behind)
        for pair in range(block // 2):
            sums = conv(following[rows], ahead, pair)
            sums = sums + conv(ordered[rows, lags * params :], behind, pair)
            put_half(sums, pair, half)

    @pl.when(plane == 0)
    def _():
        if blocks:
            newer, _, last = blocks
            windows(after(newer, last), 1, 2 * block - 2, params, fields, behind)
        for pair in range(block // 2):
            sums = conv(following[rows], ahead, pair) + conv(ordered[rows], behind, pair)
            put_half(sums, pair, half)


def lower_part(ordered, older, newer, upper, mine, theirs, ahead, times):
    block, params, fields = newer.shape
    for time in range(-1, block):
        value = newer[time] if time >= 0 else older[block - 1]
        at = block - 2 - time
        if time <= block - 2:
            times[at * params : (at + 1) * params, :fields] = value
        if time >= 0:
            times[(at + 1) * params : (at + 2) * params, fields:] = value
    for pair in range(block // 2):
        lag = (2 * pair + 2) * params
        sums = jnp.dot(
            ordered[:, :lag], times[block * params - lag :], preferred_element_type=jnp.float32
        )
        if pair < block // 2 - 1:
            sums = sums + upper[pair]
        put(sums, pair, mine, theirs)
    windows(
        after(older, newer), block + 1 - LEADING, 2 * block - 2, params, fields, ahead
    )


def head_part(*refs):
    *pieces, received, head = refs
    here = lax.axis_index("z") == 0
    each = pieces[0].shape[1]
    for time in range(head.shape[0]):
        piece = pieces[time // each]
        head[time] = jnp.where(here, piece[0, time % each], received[time])


def newer_part(*refs):
    *pieces, received, newer, last = refs
    here = lax.axis_index("z") == 0
    each = pieces[0].shape[1]
    for time in range(newer.shape[0]):
        piece = pieces[time // each]
        newer[time] = jnp.where(here, piece[0, time % each], received[time])
        last[time] = piece[1, time % each]


def pair_part(step, mine, received, *refs):
    paired = refs[-1]
    block = mine.shape[1]
    for chip in range(mine.shape[0]):
        both = mine[chip].astype(jnp.float32) + received[chip].astype(jnp.float32)
        paired[chip, step * block : (step + 1) * block] = both.astype(jnp.bfloat16)


def plane_part(arrived, summed):
    for time in range(arrived.shape[1]):
        total = arrived[0, time].astype(jnp.float32)
        for chip in range(1, arrived.shape[0]):
            total = total + arrived[chip, time].astype(jnp.float32)
        summed[time] = total.astype(jnp.bfloat16)


def ring(array, axis, by):
    size = lax.axis_size(axis)
    return lax.ppermute(array, axis, [(i, (i + by) % size) for i in range(size)])


def onward(array, axis, by):
    size = lax.axis_size(axis)
    return lax.ppermute(array, axis, [(i, i + by) for i in range(size) if 0 <= i + by < size])


def exchange(parts, axis):
    return lax.all_to_all(parts, axis, split_axis=0, concat_axis=0, tiled=True)


def observed(kernel, history, arrivals):
    block, sensors, params = kernel.shape
    steps, _, _, fields = arrivals.shape
    planes = lax.axis_size("z")
    chips = lax.axis_size("x") * lax.axis_size("y")
    pairs = (block // 2 - 1, sensors, 2 * fields)
    scratch = [pltpu.VMEM((block * params, 2 * fields), jnp.bfloat16)]
    part = jax.ShapeDtypeStruct((chips, block, planes, fields), jnp.bfloat16)

    shifted = onward(history, "z", 1)
    pieces = [arrivals] + [None] * (planes - 1)
    for source in ORDER:
        pieces[source] = lax.ppermute(arrivals, "z", [(source, 0)])

    ordered, leading, upper = pl.pallas_call(
        first_part,
        out_shape=(
            jax.ShapeDtypeStruct((sensors, block * params), jnp.bfloat16),
            jax.ShapeDtypeStruct((sensors, LEADING * params), jnp.bfloat16),
            jax.ShapeDtypeStruct(pairs, jnp.float32),
        ),
        in_specs=[VMEM, VMEM],
        out_specs=(VMEM, VMEM, VMEM),
        scratch_shapes=scratch,
        compiler_params=LIMIT,
        cost_estimate=work(2 * 10**9, 4 * 10**6),
        name="first_part",
    )(kernel, history)

    following = onward(leading, "z", -1)

    def pair(step, mine, theirs, *paired):
        received = ring(theirs, "c", 1)
        return pl.pallas_call(
            functools.partial(pair_part, step),
            out_shape=jax.ShapeDtypeStruct((chips, steps * block, planes, fields), jnp.bfloat16),
            in_specs=[VMEM] * (2 + len(paired)),
            out_specs=VMEM,
            input_output_aliases={2: 0} if paired else {},
            compiler_params=LIMIT,
            name="pair_part",
        )(mine, received, *paired)

    near = -(-(block - LEADING) // arrivals.shape[1])
    head = pl.pallas_call(
        head_part,
        out_shape=jax.ShapeDtypeStruct((block - LEADING, params, fields), jnp.bfloat16),
        in_specs=[VMEM] * (near + 1),
        out_specs=VMEM,
        compiler_params=LIMIT,
        name="head_part",
    )(*pieces[:near], shifted)
    head_twice = onward(head, "z", 1)
    newer, last = pl.pallas_call(
        newer_part,
        out_shape=(jax.ShapeDtypeStruct(shifted.shape, jnp.bfloat16),) * 2,
        in_specs=[VMEM] * (planes + 1),
        out_specs=(VMEM, VMEM),
        compiler_params=LIMIT,
        name="newer_part",
    )(*pieces, shifted)
    mine, theirs, ahead = pl.pallas_call(
        lower_part,
        out_shape=(
            part,
            part,
            jax.ShapeDtypeStruct(
                ((block - 2 + LEADING) * params, 2 * fields), jnp.bfloat16
            ),
        ),
        in_specs=[VMEM] * 4,
        out_specs=(VMEM, VMEM, VMEM),
        scratch_shapes=scratch,
        compiler_params=LIMIT,
        cost_estimate=work(2 * 10**9, 6 * 10**6),
        name="lower_part",
    )(ordered, history, newer, upper)
    paired = pair(0, mine, theirs)
    width = 2 * fields

    window = jax.ShapeDtypeStruct(((2 * block - 2) * params, width), jnp.bfloat16)

    def second(side, *blocks):
        return pl.pallas_call(
            functools.partial(second_part, side),
            out_shape=(part, window) if side else part,
            in_specs=[VMEM] * (3 + len(blocks)),
            out_specs=(VMEM, VMEM) if side else VMEM,
            compiler_params=pltpu.CompilerParams(vmem_limit_bytes=12 * 1024 * 1024),
            cost_estimate=work(2 * 10**9, 8 * 10**6),
            name="second_part",
        )(ordered, following, ahead, *blocks)

    theirs, behind = second(1, newer, head_twice, last)
    mine = second(0, behind)
    paired = pair(1, mine, theirs, paired)
    arrived = exchange(paired, ("x", "y"))
    summed = pl.pallas_call(
        plane_part,
        out_shape=jax.ShapeDtypeStruct((steps * block, planes, fields), jnp.bfloat16),
        in_specs=[VMEM],
        out_specs=VMEM,
        compiler_params=LIMIT,
        name="plane_part",
    )(arrived)
    across = exchange(jnp.moveaxis(summed, 1, 0), "z")
    across = across.astype(jnp.float32).sum(axis=0).astype(jnp.bfloat16)
    return across.reshape(steps, block, 1, fields)


def solution(mesh):
    split = Mesh(mesh.devices.reshape(mesh.shape["tm"], 4, 4, 2), EVERY)
    placed = (P("z", None, PAR), P("z", PAR, None), P(None, "z", PAR, None))
    return jax.shard_map(
        observed,
        mesh=split,
        in_specs=placed,
        out_specs=P(None, None, EVERY, None),
        check_vma=False,
    )
```

```python
import functools

import jax
import jax.numpy as jnp
from jax import lax
from jax.experimental import pallas as pl
from jax.experimental.pallas import tpu as pltpu
from jax.sharding import Mesh
from jax.sharding import PartitionSpec as P

ORDER = (5, 6, 7, 4, 3, 2, 1)
LEADING = 8
PAR = ("x", "y", "c")
EVERY = ("z", "x", "y", "c")
VMEM = pl.BlockSpec(memory_space=pltpu.VMEM)
LIMIT = pltpu.CompilerParams(vmem_limit_bytes=8 * 1024 * 1024)


def work(flops, nbytes):
    return pl.CostEstimate(flops=flops, bytes_accessed=nbytes, transcendentals=0)


def upper_part(ordered, older, upper, times):
    block, params, fields = older.shape
    last = block - 2
    for time in range(1, block):
        if time <= last:
            times[(last - time) * params : (last - time + 1) * params, :fields] = older[time]
        if time >= 2:
            at = last + 1 - time
            times[at * params : (at + 1) * params, fields:] = older[time]
    for pair in range(block // 2 - 1):
        lag = (2 * pair + 2) * params
        upper[pair] = jnp.dot(
            ordered[:, lag:], times[: block * params - lag], preferred_element_type=jnp.float32
        )


def order_rows(kernel, ordered):
    lags, sensors, params = kernel.shape
    planes = 8
    half = sensors // 2
    row = lax.broadcasted_iota(jnp.int32, (sensors, sensors), 0)
    col = lax.broadcasted_iota(jnp.int32, (sensors, sensors), 1)
    other = (row >= half).astype(jnp.int32)
    place = row - half * other
    core = lax.axis_index("c")
    parity = core + other - 2 * core * other
    sensor = (place % planes) * (sensors // planes) + (place // planes) * 2 + parity
    select = (col == sensor).astype(jnp.bfloat16)
    for lag in range(lags):
        rows = jnp.dot(select, kernel[lag], preferred_element_type=jnp.float32)
        ordered[:, lag * params : (lag + 1) * params] = rows.astype(jnp.bfloat16)


def first_part(kernel, older, ordered, leading, upper, times):
    order_rows(kernel, ordered)
    leading[...] = ordered[:, : leading.shape[1]]
    upper_part(ordered, older, upper, times)


def windows(value, low, high, params, fields, times):
    for time in range(low, high + 2):
        if time <= high:
            times[(high - time) * params : (high - time + 1) * params, :fields] = value(time)
        if time > low:
            at = high + 1 - time
            times[at * params : (at + 1) * params, fields:] = value(time)


def after(first, then):
    block = first.shape[0]
    return lambda time: first[time] if time < block else then[time - block]


def product(left, right, start):
    window = right[start : start + left.shape[1]]
    return jnp.dot(left, window, preferred_element_type=jnp.float32)


def put_half(sums, pair, half):
    fields = sums.shape[1] // 2
    sums = sums.astype(jnp.bfloat16)
    for odd in range(2):
        part = sums[:, odd * fields : (odd + 1) * fields]
        half[:, 2 * pair + odd] = part.reshape(half.shape[0], half.shape[2], fields)


def put(sums, pair, mine, theirs):
    count = sums.shape[0] // 2
    put_half(sums[:count], pair, mine)
    put_half(sums[count:], pair, theirs)


def second_part(side, ordered, following, ahead, newer, head, last, half, behind, arrivals):
    block, params, fields = newer.shape
    lags = following.shape[1] // params
    plane = lax.axis_index("z")
    count = ordered.shape[0] // 2
    rows = slice(side * count, (side + 1) * count)

    def conv(left, right, pair):
        return product(left, right, (block - 2 - 2 * pair) * params)

    @pl.when(plane != 0)
    def _():
        windows(after(newer, head), 1, 2 * block - 2 - lags, params, fields, behind)
        for pair in range(block // 2):
            sums = conv(following[rows], ahead, pair)
            sums = sums + conv(ordered[rows, lags * params :], behind, pair)
            put_half(sums, pair, half)

    @pl.when(plane == 0)
    def _():
        windows(after(newer, last), 1, 2 * block - 2, params, fields, arrivals)
        for pair in range(block // 2):
            sums = conv(following[rows], ahead, pair) + conv(ordered[rows], arrivals, pair)
            put_half(sums, pair, half)


def lower_part(ordered, older, newer, upper, mine, theirs, ahead, times):
    block, params, fields = newer.shape
    for time in range(-1, block):
        value = newer[time] if time >= 0 else older[block - 1]
        at = block - 2 - time
        if time <= block - 2:
            times[at * params : (at + 1) * params, :fields] = value
        if time >= 0:
            times[(at + 1) * params : (at + 2) * params, fields:] = value
    for pair in range(block // 2):
        lag = (2 * pair + 2) * params
        sums = jnp.dot(
            ordered[:, :lag], times[block * params - lag :], preferred_element_type=jnp.float32
        )
        if pair < block // 2 - 1:
            sums = sums + upper[pair]
        put(sums, pair, mine, theirs)
    windows(
        after(older, newer), block + 1 - LEADING, 2 * block - 2, params, fields, ahead
    )


def head_part(*refs):
    *pieces, received, head = refs
    here = lax.axis_index("z") == 0
    each = pieces[0].shape[1]
    for time in range(head.shape[0]):
        piece = pieces[time // each]
        head[time] = jnp.where(here, piece[0, time % each], received[time])


def newer_part(*refs):
    *pieces, received, newer, last = refs
    here = lax.axis_index("z") == 0
    each = pieces[0].shape[1]
    for time in range(newer.shape[0]):
        piece = pieces[time // each]
        newer[time] = jnp.where(here, piece[0, time % each], received[time])
        last[time] = piece[1, time % each]


def pair_part(step, mine, received, *refs):
    paired = refs[-1]
    block = mine.shape[1]
    for chip in range(mine.shape[0]):
        both = mine[chip].astype(jnp.float32) + received[chip].astype(jnp.float32)
        paired[chip, step * block : (step + 1) * block] = both.astype(jnp.bfloat16)


def plane_part(arrived, summed):
    for time in range(arrived.shape[1]):
        total = arrived[0, time].astype(jnp.float32)
        for chip in range(1, arrived.shape[0]):
            total = total + arrived[chip, time].astype(jnp.float32)
        summed[time] = total.astype(jnp.bfloat16)


def ring(array, axis, by):
    size = lax.axis_size(axis)
    return lax.ppermute(array, axis, [(i, (i + by) % size) for i in range(size)])


def onward(array, axis, by):
    size = lax.axis_size(axis)
    return lax.ppermute(array, axis, [(i, i + by) for i in range(size) if 0 <= i + by < size])


def exchange(parts, axis):
    return lax.all_to_all(parts, axis, split_axis=0, concat_axis=0, tiled=True)


def observed(kernel, history, arrivals):
    block, sensors, params = kernel.shape
    steps, _, _, fields = arrivals.shape
    planes = lax.axis_size("z")
    chips = lax.axis_size("x") * lax.axis_size("y")
    pairs = (block // 2 - 1, sensors, 2 * fields)
    scratch = [pltpu.VMEM((block * params, 2 * fields), jnp.bfloat16)]
    part = jax.ShapeDtypeStruct((chips, block, planes, fields), jnp.bfloat16)

    shifted = onward(history, "z", 1)
    pieces = [arrivals] + [None] * (planes - 1)
    for source in ORDER:
        pieces[source] = lax.ppermute(arrivals, "z", [(source, 0)])

    ordered, leading, upper = pl.pallas_call(
        first_part,
        out_shape=(
            jax.ShapeDtypeStruct((sensors, block * params), jnp.bfloat16),
            jax.ShapeDtypeStruct((sensors, LEADING * params), jnp.bfloat16),
            jax.ShapeDtypeStruct(pairs, jnp.float32),
        ),
        in_specs=[VMEM, VMEM],
        out_specs=(VMEM, VMEM, VMEM),
        scratch_shapes=scratch,
        compiler_params=LIMIT,
        cost_estimate=work(2 * 10**9, 4 * 10**6),
        name="first_part",
    )(kernel, history)

    following = onward(leading, "z", -1)

    def pair(step, mine, theirs, *paired):
        received = ring(theirs, "c", 1)
        return pl.pallas_call(
            functools.partial(pair_part, step),
            out_shape=jax.ShapeDtypeStruct((chips, steps * block, planes, fields), jnp.bfloat16),
            in_specs=[VMEM] * (2 + len(paired)),
            out_specs=VMEM,
            input_output_aliases={2: 0} if paired else {},
            compiler_params=LIMIT,
            name="pair_part",
        )(mine, received, *paired)

    near = -(-(block - LEADING) // arrivals.shape[1])
    head = pl.pallas_call(
        head_part,
        out_shape=jax.ShapeDtypeStruct((block - LEADING, params, fields), jnp.bfloat16),
        in_specs=[VMEM] * (near + 1),
        out_specs=VMEM,
        compiler_params=LIMIT,
        name="head_part",
    )(*pieces[:near], shifted)
    head_twice = onward(head, "z", 1)
    newer, last = pl.pallas_call(
        newer_part,
        out_shape=(jax.ShapeDtypeStruct(shifted.shape, jnp.bfloat16),) * 2,
        in_specs=[VMEM] * (planes + 1),
        out_specs=(VMEM, VMEM),
        compiler_params=LIMIT,
        name="newer_part",
    )(*pieces, shifted)
    mine, theirs, ahead = pl.pallas_call(
        lower_part,
        out_shape=(
            part,
            part,
            jax.ShapeDtypeStruct(
                ((block - 2 + LEADING) * params, 2 * fields), jnp.bfloat16
            ),
        ),
        in_specs=[VMEM] * 4,
        out_specs=(VMEM, VMEM, VMEM),
        scratch_shapes=scratch,
        compiler_params=LIMIT,
        cost_estimate=work(2 * 10**9, 6 * 10**6),
        name="lower_part",
    )(ordered, history, newer, upper)
    paired = pair(0, mine, theirs)
    width = 2 * fields

    def second(side):
        return pl.pallas_call(
            functools.partial(second_part, side),
            out_shape=part,
            in_specs=[VMEM] * 6,
            out_specs=VMEM,
            scratch_shapes=[
                pltpu.VMEM(((2 * block - 2 - LEADING) * params, width), jnp.bfloat16),
                pltpu.VMEM(((2 * block - 2) * params, width), jnp.bfloat16),
            ],
            compiler_params=pltpu.CompilerParams(vmem_limit_bytes=12 * 1024 * 1024),
            cost_estimate=work(2 * 10**9, 8 * 10**6),
            name="second_part",
        )(ordered, following, ahead, newer, head_twice, last)

    theirs = second(1)
    mine = second(0)
    paired = pair(1, mine, theirs, paired)
    arrived = exchange(paired, ("x", "y"))
    summed = pl.pallas_call(
        plane_part,
        out_shape=jax.ShapeDtypeStruct((steps * block, planes, fields), jnp.bfloat16),
        in_specs=[VMEM],
        out_specs=VMEM,
        compiler_params=LIMIT,
        name="plane_part",
    )(arrived)
    across = exchange(jnp.moveaxis(summed, 1, 0), "z")
    across = across.astype(jnp.float32).sum(axis=0).astype(jnp.bfloat16)
    return across.reshape(steps, block, 1, fields)


def solution(mesh):
    split = Mesh(mesh.devices.reshape(mesh.shape["tm"], 4, 4, 2), EVERY)
    placed = (P("z", None, PAR), P("z", PAR, None), P(None, "z", PAR, None))
    return jax.shard_map(
        observed,
        mesh=split,
        in_specs=placed,
        out_specs=P(None, None, EVERY, None),
        check_vma=False,
    )
```
